64 devices in a mesh: rep: 8 (over x, y, core), dp: 8 (over z).
Axes of the slice: x: 2, y: 2, z: 8, core: 2. Of those that a mesh axis runs over, the one named last changes fastest.
The devices are a block of a 4x4x8 slice.
Arguments:
- x: bfloat16 [64, 2048, 768], P(('rep', 'dp')), parts along dimension 0
- dy: bfloat16 [64, 2048, 768], P(('rep', 'dp')), parts along dimension 0
- w_gate: bfloat16 [2, 768, 2048], replicated
- w_up: bfloat16 [2, 768, 2048], replicated
- w_down: bfloat16 [2, 2048, 768], replicated
- m_w_gate: float32 [2, 768, 2048], replicated
- m_w_up: float32 [2, 768, 2048], replicated
- m_w_down: float32 [2, 2048, 768], replicated
- v_w_gate: float32 [2, 768, 2048], replicated
- v_w_up: float32 [2, 768, 2048], replicated
- v_w_down: float32 [2, 2048, 768], replicated
Outputs:
- output 1: bfloat16 [16, 768, 2048], P('rep'), parts along dimension 0
- output 2: bfloat16 [16, 768, 2048], P('rep'), parts along dimension 0
- output 3: bfloat16 [16, 2048, 768], P('rep'), parts along dimension 0
- output 4: float32 [16, 768, 2048], P('rep'), parts along dimension 0
- output 5: float32 [16, 768, 2048], P('rep'), parts along dimension 0
- output 6: float32 [16, 2048, 768], P('rep'), parts along dimension 0
- output 7: float32 [16, 768, 2048], P('rep'), parts along dimension 0
- output 8: float32 [16, 768, 2048], P('rep'), parts along dimension 0
- output 9: float32 [16, 2048, 768], P('rep'), parts along dimension 0
There are 8 independent parts. The reference program is written for one: setup_inputs(seed, part) draws one part's arguments, and reference() takes and returns one part's arrays. A program takes and returns all parts, laid end to end along the dimension named above; an argument that names none is the same for every part.
All inputs are finite; a program needn't handle non-finite values.
Results may differ from the reference program's by a relative error of at most 0.02.
Values are sent between devices in bfloat16 or wider.
A program may use at most 768 MiB of HBM per device.

```python
import jax
import jax.numpy as jnp
from jax import lax

SEQUENCES = 8
TOKENS = 2048
D = 768
FF = 2048
LAYERS = 2
NAMES = ("w_gate", "w_up", "w_down")
SHAPES = {"w_gate": (LAYERS, D, FF), "w_up": (LAYERS, D, FF), "w_down": (LAYERS, FF, D)}


def bump(key, n, height):
    away = (jnp.arange(n, dtype=jnp.int32) - jax.random.randint(key, (), 0, n, jnp.int32)) % n
    return jnp.where(away < n // 8, height, 1.0)


def together(key, own, strength):
    shared = jax.random.normal(key, own.shape[1:], jnp.float32)
    return (own + strength * shared) * lax.rsqrt(1 + strength * strength)


def setup_inputs(seed: int = 0, part: int = 0) -> dict:
    kx, kdy, ka, kb, kz, kf, kh, kl, *keys = jax.random.split(jax.random.key(seed), 8 + 3 * len(NAMES))
    kx, kdy, ka, kb = (jax.random.fold_in(k, part) for k in (kx, kdy, ka, kb))
    kw, km, kv = (keys[i::3] for i in range(3))
    shape = (SEQUENCES, TOKENS, D)
    much_x, much_dy = jax.random.uniform(kz, (2,), jnp.float32, 0.0, 1.0)
    loud = 2.0 ** jax.random.uniform(jax.random.fold_in(kz, 1), (), jnp.float32, -1.0, 2.0)
    layers = 2.0 ** jax.random.uniform(kl, (LAYERS, 1, 1), jnp.float32, -1.0, 1.0)
    x = together(ka, jax.random.normal(kx, shape, jnp.float32), much_x) * bump(kf, D, 4.0)
    dy = together(kb, jax.random.normal(kdy, shape, jnp.float32), much_dy)
    drawn = {"x": x.astype(jnp.bfloat16), "dy": (loud * dy * (SEQUENCES * TOKENS) ** -0.5).astype(jnp.bfloat16)}
    for key, name in zip(kw, NAMES, strict=True):
        w = jax.random.normal(key, SHAPES[name], jnp.float32) * SHAPES[name][1] ** -0.5
        drawn[name] = (w * {"w_gate": 1.0, "w_up": bump(kh, FF, 4.0), "w_down": layers}[name]).astype(jnp.bfloat16)
    for key, name in zip(km, NAMES, strict=True):
        drawn[f"m_{name}"] = 0.1 * jax.random.normal(key, SHAPES[name], jnp.float32)
    for key, name in zip(kv, NAMES, strict=True):
        drawn[f"v_{name}"] = jax.random.uniform(key, SHAPES[name], jnp.float32, 0.005, 0.015)
    return drawn


def matmul(a, w):
    return jnp.dot(a, w, preferred_element_type=jnp.float32).astype(jnp.bfloat16)


def normed(h):
    wide = h.astype(jnp.float32)
    scale = lax.rsqrt(jnp.mean(wide**2, -1, keepdims=True) + 1e-6)
    return (wide * scale).astype(jnp.bfloat16)


def layer(h, w):
    a = normed(h)
    gate = jnp.dot(a, w["w_gate"], preferred_element_type=jnp.float32)
    up = jnp.dot(a, w["w_up"], preferred_element_type=jnp.float32)
    return h + matmul((jax.nn.silu(gate) * up).astype(jnp.bfloat16), w["w_down"])


def adamw(w, m, v, g):
    m = 0.9 * m + 0.1 * g
    v = 0.95 * v + 0.05 * g * g
    step = m * lax.rsqrt(v + 1e-8) + 0.1 * w
    return (w - 0.02 * step).astype(jnp.bfloat16), m, v


def stack(weights, h):
    return lax.scan(lambda h, w: (layer(h, w), None), h, weights)[0]


def reference(x, dy, w_gate, w_up, w_down, m_w_gate, m_w_up, m_w_down, v_w_gate, v_w_up, v_w_down):
    weights = dict(zip(NAMES, (w_gate, w_up, w_down), strict=True))

    def take(so_far, sequence):
        h, by_y = sequence
        _, back = jax.vjp(lambda w: stack(w, h), weights)
        return jax.tree.map(lambda total, term: total + term.astype(jnp.float32), so_far, back(by_y)[0]), None

    none_yet = {name: jnp.zeros(w.shape, jnp.float32) for name, w in weights.items()}
    by_weights, _ = lax.scan(take, none_yet, (x, dy))
    gradients = [by_weights[name].astype(jnp.bfloat16).astype(jnp.float32) for name in NAMES]
    new = [
        adamw(w.astype(jnp.float32), m, v, g)
        for w, m, v, g in zip((w_gate, w_up, w_down), (m_w_gate, m_w_up, m_w_down), (v_w_gate, v_w_up, v_w_down), gradients, strict=True)
    ]
    return tuple(one[which] for which in range(3) for one in new)
```

```python
import functools

import jax
import jax.numpy as jnp
from jax import lax
from jax.experimental import pallas as pl
from jax.experimental.pallas import tpu as pltpu
from jax.sharding import PartitionSpec as P

F32, BF16 = jnp.float32, jnp.bfloat16
LIMIT = 60 * 1024 * 1024
ROWS = 512
CUT = 512
TILE = 256
DIRECT = 2
NT = (((1,), (1,)), ((), ()))


def dot(a, b):
    return jnp.dot(a, b, preferred_element_type=F32)


def dot_nt(a, b):
    return lax.dot_general(a, b, NT, preferred_element_type=F32)


def scale_of(wide):
    return lax.rsqrt(jnp.mean(wide * wide, -1, keepdims=True) + 1e-6)


def forward_kernel(x_ref, dy_ref, wg_ref, wu_ref, wd_ref, h_ref, a1_ref, a1t_ref, a0_ref, a0t_ref, dyt_ref, act):
    wide = x_ref[0].astype(F32)
    a0 = (wide * scale_of(wide)).astype(BF16)
    a0_ref[...] = a0
    ff = wg_ref.shape[2]
    for f in range(0, ff, CUT):
        gate = dot(a0, wg_ref[0, :, f : f + CUT])
        up = dot(a0, wu_ref[0, :, f : f + CUT])
        act[:, f : f + CUT] = (gate * jax.nn.sigmoid(gate) * up).astype(BF16)
    a0t_ref[...] = a0.T
    dyt_ref[...] = dy_ref[0].T
    h = x_ref[0] + dot(act[...], wd_ref[0]).astype(BF16)
    h_ref[...] = h
    wide = h.astype(F32)
    a1 = (wide * scale_of(wide)).astype(BF16)
    a1_ref[...] = a1
    a1t_ref[...] = a1.T


def forward(x, dy, wg, wu, wd, layer):
    _, tokens, d = x.shape
    ff = wg.shape[2]
    weight = lambda w: pl.BlockSpec((1,) + w.shape[1:], lambda i: (layer, 0, 0))
    seq = pl.BlockSpec((1, ROWS, d), lambda i: (0, i, 0))
    flat = pl.BlockSpec((ROWS, d), lambda i: (i, 0))
    turned = pl.BlockSpec((d, ROWS), lambda i: (0, i))
    plain, turn = jax.ShapeDtypeStruct((tokens, d), BF16), jax.ShapeDtypeStruct((d, tokens), BF16)
    return pl.pallas_call(
        forward_kernel,
        grid=(tokens // ROWS,),
        in_specs=[seq, seq, weight(wg), weight(wu), weight(wd)],
        out_specs=[flat, flat, turned, flat, turned, turned],
        out_shape=[plain, plain, turn, plain, turn, turn],
        scratch_shapes=[pltpu.VMEM((ROWS, ff), BF16)],
        compiler_params=pltpu.CompilerParams(vmem_limit_bytes=LIMIT),
        cost_estimate=pl.CostEstimate(flops=6 * tokens * d * ff, bytes_accessed=16 * tokens * d + 6 * d * ff, transcendentals=tokens * ff),
        name="forward",
    )(x, dy, wg, wu, wd)


def rdma(n, me, d, s, slot, own, landed, send_sem, recv_sem):
    turn = 1 - 2 * d
    shard = lax.rem(me - turn * s + 2 * n, n)
    high = own.shape[1] // (2 * n)
    mine = own.at[slot, pl.ds(pl.multiple_of((2 * shard + d) * high, 16), high), :]
    return mine, pltpu.make_async_remote_copy(
        src_ref=mine,
        dst_ref=landed.at[d, slot, s] if s < n - 1 else mine,
        send_sem=send_sem.at[d, slot],
        recv_sem=recv_sem.at[d, slot, s],
        device_id={"dp": lax.rem(me + turn + n, n)},
        device_id_type=pl.DeviceIdType.MESH,
    )


def backward_kernel(n, ringed, *refs):
    a1_in, a1t_in, dy_in, dyt_in, h_in, a0_in, a0t_in, wg_in, wu_in, wd_in = refs[:10]
    ring_out, direct_out = refs[10:12]
    a, at, dy, dyt, by_gate, by_up, own, landed, act, dgate, dup, wg, wu, wd = refs[12:26]
    load_sem, weight_sem, out_sem, send_sem, recv_sem = refs[26:]
    tokens, d_model = a.shape
    per = wg_in.shape[2] // TILE
    pieces = 2 * per
    me = lax.axis_index("dp")
    barrier = pltpu.get_barrier_semaphore()
    for other in (1, n - 1):
        pl.semaphore_signal(barrier, inc=1, device_id={"dp": lax.rem(me + other, n)}, device_id_type=pl.DeviceIdType.MESH)

    def load(pairs):
        copies = [pltpu.make_async_copy(src, dst, load_sem.at[i]) for i, (src, dst) in enumerate(pairs)]
        for copy in copies:
            copy.start()
        for copy in copies:
            copy.wait()

    def tiles(piece):
        which, slot = 1 - piece // per, lax.rem(piece, 2)
        here = pl.ds(pl.multiple_of(lax.rem(piece, per) * TILE, TILE), TILE)
        return [
            pltpu.make_async_copy(wg_in.at[which, :, here], wg.at[slot], weight_sem.at[slot, 0]),
            pltpu.make_async_copy(wu_in.at[which, :, here], wu.at[slot], weight_sem.at[slot, 1]),
            pltpu.make_async_copy(wd_in.at[which, here, :], wd.at[slot], weight_sem.at[slot, 2]),
        ]

    for copy in tiles(0):
        copy.start()
    load([(a1_in, a), (dy_in.at[0], dy), (a1t_in, at), (dyt_in, dyt)])
    by_gate[...] = jnp.zeros_like(by_gate)
    by_up[...] = jnp.zeros_like(by_up)
    pl.semaphore_wait(barrier, 2)

    def serve(turn, odd):
        for age in reversed(range(odd, n)):
            s = 2 * age - odd
            piece = turn - age

            @pl.when(jnp.logical_and(piece >= 0, piece < ringed))
            def _():
                slot = lax.rem(piece, n)
                for d in range(2):
                    if s:
                        before = rdma(n, me, d, s - 1, slot, own, landed, send_sem, recv_sem)[1]
                        before.wait_recv()
                        before.wait_send()
                    if s < 2 * n - 2:
                        mine, copy = rdma(n, me, d, s, slot, own, landed, send_sem, recv_sem)
                        if 0 < s < n:
                            mine[...] = (mine[...].astype(F32) + landed[d, slot, s - 1].astype(F32)).astype(BF16)
                        copy.start()
                if s == 2 * n - 2:
                    pltpu.make_async_copy(own.at[slot], ring_out.at[piece], out_sem.at[slot]).start()

    @pl.loop(0, max(pieces, ringed + n - 1))
    def _(turn):
        busy = turn < pieces
        slot = lax.rem(turn, n)
        now = lax.rem(turn, 2)

        @pl.when(turn == per)
        def _():
            load([(h_in, a)])

            @pl.loop(0, tokens // TILE)
            def _(c):
                here = pl.ds(pl.multiple_of(c * TILE, TILE), TILE)
                by_a = (by_gate[here, :].astype(BF16) + by_up[here, :].astype(BF16)).astype(F32)
                wide = a[here, :].astype(F32)
                scale = scale_of(wide)
                along = jnp.mean(by_a * wide, -1, keepdims=True)
                by_h = (by_a * scale - wide * (scale * scale * scale * along)).astype(BF16) + dy[here, :]
                dy[here, :] = by_h
                dyt[:, here] = by_h.T

            load([(a0_in, a), (a0t_in, at)])

        @pl.when(busy)
        def _():
            for copy in tiles(turn):
                copy.wait()

            @pl.when(turn + 1 < pieces)
            def _():
                for copy in tiles(turn + 1):
                    copy.start()

            @pl.loop(0, tokens // ROWS)
            def _(c):
                here = pl.ds(pl.multiple_of(c * ROWS, ROWS), ROWS)
                gate = dot(a[here, :], wg[now])
                up = dot(a[here, :], wu[now])
                by_act = dot_nt(dy[here, :], wd[now]).astype(BF16).astype(F32)
                sig = jax.nn.sigmoid(gate)
                silu = gate * sig
                act[here, :] = (silu * up).astype(BF16)
                dup[here, :] = (by_act * silu).astype(BF16)
                dgate[here, :] = (by_act * up * (sig + silu * (1 - sig))).astype(BF16)

        serve(turn, 1)

        @pl.when(busy)
        def _():
            @pl.when(turn >= n)
            def _():
                pltpu.make_async_copy(own.at[slot], ring_out.at[0], out_sem.at[slot]).wait()

            own[slot, :d_model, :] = dot(at[...], dgate[...]).astype(BF16)
            own[slot, d_model : 2 * d_model, :] = dot(at[...], dup[...]).astype(BF16)
            down = dot(dyt[...], act[...]).astype(BF16).T
            for i in range(d_model // TILE):
                own[slot, 2 * d_model + i * TILE : 2 * d_model + (i + 1) * TILE, :] = down[:, i * TILE : (i + 1) * TILE]

            @pl.when(turn >= ringed)
            def _():
                pltpu.make_async_copy(own.at[slot], direct_out.at[turn - ringed], out_sem.at[slot]).start()

        serve(turn, 0)

        @pl.when(turn < per)
        def _():
            @pl.loop(0, tokens // ROWS)
            def _(c):
                here = pl.ds(pl.multiple_of(c * ROWS, ROWS), ROWS)
                by_gate[here, :] += dot_nt(dgate[here, :], wg[now])
                by_up[here, :] += dot_nt(dup[here, :], wu[now])

    for slot in range(n):
        pltpu.make_async_copy(own.at[slot], ring_out.at[0], out_sem.at[slot]).wait()


def backward(n, x, dy, h1, a1, a1t, a0, a0t, dyt, wg, wu, wd):
    tokens, d = a1.shape
    ff = wg.shape[2]
    pieces = 2 * ff // TILE
    ringed = pieces - DIRECT
    high = 3 * d // (2 * n)
    anywhere = pl.BlockSpec(memory_space=pl.ANY)
    return pl.pallas_call(
        functools.partial(backward_kernel, n, ringed),
        in_specs=[anywhere] * 10,
        out_specs=[anywhere] * 2,
        out_shape=[jax.ShapeDtypeStruct((ringed, 3 * d, TILE), BF16), jax.ShapeDtypeStruct((DIRECT, 3 * d, TILE), BF16)],
        scratch_shapes=[
            pltpu.VMEM((tokens, d), BF16),
            pltpu.VMEM((d, tokens), BF16),
            pltpu.VMEM((tokens, d), BF16),
            pltpu.VMEM((d, tokens), BF16),
            pltpu.VMEM((tokens, d), F32),
            pltpu.VMEM((tokens, d), F32),
            pltpu.VMEM((n, 3 * d, TILE), BF16),
            pltpu.VMEM((2, n, n - 1, high, TILE), BF16),
            pltpu.VMEM((tokens, TILE), BF16),
            pltpu.VMEM((tokens, TILE), BF16),
            pltpu.VMEM((tokens, TILE), BF16),
            pltpu.VMEM((2, d, TILE), BF16),
            pltpu.VMEM((2, d, TILE), BF16),
            pltpu.VMEM((2, TILE, d), BF16),
            pltpu.SemaphoreType.DMA((4,)),
            pltpu.SemaphoreType.DMA((2, 3)),
            pltpu.SemaphoreType.DMA((n,)),
            pltpu.SemaphoreType.DMA((2, n)),
            pltpu.SemaphoreType.DMA((2, n, 2 * n - 2)),
        ],
        compiler_params=pltpu.CompilerParams(vmem_limit_bytes=63 * 1024 * 1024, collective_id=0, has_side_effects=True),
        cost_estimate=pl.CostEstimate(flops=28 * tokens * d * ff, bytes_accessed=40 * d * ff, transcendentals=2 * tokens * ff),
        name="backward",
    )(a1, a1t, dy, dyt, h1, a0, a0t, wg, wu, wd)


def adamw_kernel(*refs):
    ins, g_ref, outs = refs[:9], refs[9], refs[-9:]
    d = ins[0].shape[1]
    for i in range(3):
        w, m, v = (ins[3 * k + i] for k in range(3))
        if i < 2:
            g = g_ref[0, i * d : (i + 1) * d, :].astype(F32)
        else:
            g = jnp.concatenate([g_ref[0, at : at + TILE, :].astype(F32) for at in range(2 * d, 3 * d, TILE)], axis=1)
        new_m = 0.9 * m[0] + 0.1 * g
        new_v = 0.95 * v[0] + 0.05 * g * g
        step = new_m * lax.rsqrt(new_v + 1e-8) + 0.1 * w[0].astype(F32)
        outs[i][0] = (w[0].astype(F32) - 0.02 * step).astype(BF16)
        outs[3 + i][0] = new_m
        outs[6 + i][0] = new_v


def adamw(weights, ms, vs, g, so_far, first):
    d, ff = weights[0].shape[1:]
    per = ff // TILE
    which = lambda i: 1 - (first + i) // per
    col = pl.BlockSpec((1, d, TILE), lambda i: (which(i), 0, (first + i) % per))
    row = pl.BlockSpec((1, TILE, d), lambda i: (which(i), (first + i) % per, 0))
    three = [col, col, row]
    old = list(so_far or ())
    count = g.size
    return pl.pallas_call(
        adamw_kernel,
        grid=(g.shape[0],),
        in_specs=three * 3 + [pl.BlockSpec((1, 3 * d, TILE), lambda i: (i, 0, 0))] + [pl.BlockSpec(memory_space=pl.ANY)] * len(old),
        out_specs=three * 3,
        out_shape=[jax.ShapeDtypeStruct(v.shape, v.dtype) for v in (*weights, *ms, *vs)],
        input_output_aliases={10 + i: i for i in range(len(old))},
        compiler_params=pltpu.CompilerParams(vmem_limit_bytes=LIMIT),
        cost_estimate=pl.CostEstimate(flops=15 * count, bytes_accessed=22 * count, transcendentals=count),
        name=f"adamw_{first}",
    )(*weights, *ms, *vs, g, *old)


def solution(mesh):
    n = mesh.shape["dp"]

    def step(x, dy, *arrays):
        weights, ms, vs = (arrays[i : i + 3] for i in (0, 3, 6))
        wg, wu, wd = weights
        h1, a1, a1t, a0, a0t, dyt = forward(x, dy, wg, wu, wd, 0)
        ring, direct = backward(n, x, dy, h1, a1, a1t, a0, a0t, dyt, wg, wu, wd)
        direct = lax.psum(direct, "dp")
        so_far = adamw(weights, ms, vs, ring, None, 0)
        return tuple(adamw(weights, ms, vs, direct, so_far, ring.shape[0]))

    return jax.shard_map(
        step,
        mesh=mesh,
        in_specs=(P(("rep", "dp"), None, None),) * 2 + (P(None, None, None),) * 9,
        out_specs=(P("rep", None, None),) * 9,
        check_vma=False,
    )
```

```python
import functools

import jax
import jax.numpy as jnp
from jax import lax
from jax.experimental import pallas as pl
from jax.experimental.pallas import tpu as pltpu
from jax.sharding import PartitionSpec as P

F32, BF16 = jnp.float32, jnp.bfloat16
LIMIT = 60 * 1024 * 1024
ROWS = 512
CUT = 512
TILE = 256
DIRECT = 4
NT = (((1,), (1,)), ((), ()))


def dot(a, b):
    return jnp.dot(a, b, preferred_element_type=F32)


def dot_nt(a, b):
    return lax.dot_general(a, b, NT, preferred_element_type=F32)


def scale_of(wide):
    return lax.rsqrt(jnp.mean(wide * wide, -1, keepdims=True) + 1e-6)


def forward_kernel(x_ref, dy_ref, wg_ref, wu_ref, wd_ref, h_ref, a1_ref, a1t_ref, a0_ref, a0t_ref, dyt_ref, act):
    wide = x_ref[0].astype(F32)
    a0 = (wide * scale_of(wide)).astype(BF16)
    a0_ref[...] = a0
    ff = wg_ref.shape[2]
    for f in range(0, ff, CUT):
        gate = dot(a0, wg_ref[0, :, f : f + CUT])
        up = dot(a0, wu_ref[0, :, f : f + CUT])
        act[:, f : f + CUT] = (gate * jax.nn.sigmoid(gate) * up).astype(BF16)
    a0t_ref[...] = a0.T
    dyt_ref[...] = dy_ref[0].T
    h = x_ref[0] + dot(act[...], wd_ref[0]).astype(BF16)
    h_ref[...] = h
    wide = h.astype(F32)
    a1 = (wide * scale_of(wide)).astype(BF16)
    a1_ref[...] = a1
    a1t_ref[...] = a1.T


def forward(x, dy, wg, wu, wd, layer):
    _, tokens, d = x.shape
    ff = wg.shape[2]
    weight = lambda w: pl.BlockSpec((1,) + w.shape[1:], lambda i: (layer, 0, 0))
    seq = pl.BlockSpec((1, ROWS, d), lambda i: (0, i, 0))
    flat = pl.BlockSpec((ROWS, d), lambda i: (i, 0))
    turned = pl.BlockSpec((d, ROWS), lambda i: (0, i))
    plain, turn = jax.ShapeDtypeStruct((tokens, d), BF16), jax.ShapeDtypeStruct((d, tokens), BF16)
    return pl.pallas_call(
        forward_kernel,
        grid=(tokens // ROWS,),
        in_specs=[seq, seq, weight(wg), weight(wu), weight(wd)],
        out_specs=[flat, flat, turned, flat, turned, turned],
        out_shape=[plain, plain, turn, plain, turn, turn],
        scratch_shapes=[pltpu.VMEM((ROWS, ff), BF16)],
        compiler_params=pltpu.CompilerParams(vmem_limit_bytes=LIMIT),
        cost_estimate=pl.CostEstimate(flops=6 * tokens * d * ff, bytes_accessed=16 * tokens * d + 6 * d * ff, transcendentals=tokens * ff),
        name="forward",
    )(x, dy, wg, wu, wd)


def ring_rows(n, me, d, s, slot, own):
    shard = lax.rem(me - (1 - 2 * d) * s + 2 * n, n)
    high = own.shape[1] // (2 * n)
    return own.at[slot, pl.ds(pl.multiple_of((2 * shard + d) * high, 16), high), :]


def ring_copy(n, me, d, s, *, slot, own, landed, send_sem, recv_sem, whole):
    mine = ring_rows(n, me, d, s, slot, own)
    return pltpu.make_async_remote_copy(
        src_ref=mine,
        dst_ref=mine if whole else landed.at[d, slot, s],
        send_sem=send_sem.at[d, slot],
        recv_sem=recv_sem.at[d, slot, s],
        device_id={"dp": lax.rem(me + 1 - 2 * d + n, n)},
        device_id_type=pl.DeviceIdType.MESH,
    )


def backward_kernel(n, ringed, *refs):
    a1_in, a1t_in, dy_in, dyt_in, h_in, a0_in, a0t_in, wg_in, wu_in, wd_in = refs[:10]
    ring_out, direct_out = refs[10:12]
    a, at, dy, dyt, by_gate, by_up, own, landed, act, dgate, dup, wg, wu, wd = refs[12:26]
    load_sem, weight_sem, out_sem, direct_sem, send_sem, recv_sem = refs[26:]
    tokens, d_model = a.shape
    per = wg_in.shape[2] // TILE
    pieces = 2 * per
    me = lax.axis_index("dp")
    barrier = pltpu.get_barrier_semaphore()
    for other in (1, n - 1):
        pl.semaphore_signal(barrier, inc=1, device_id={"dp": lax.rem(me + other, n)}, device_id_type=pl.DeviceIdType.MESH)

    def tiles(piece):
        which, slot = 1 - piece // per, lax.rem(piece, 2)
        here = pl.ds(pl.multiple_of(lax.rem(piece, per) * TILE, TILE), TILE)
        return [
            pltpu.make_async_copy(wg_in.at[which, :, here], wg.at[slot], weight_sem.at[slot, 0]),
            pltpu.make_async_copy(wu_in.at[which, :, here], wu.at[slot], weight_sem.at[slot, 1]),
            pltpu.make_async_copy(wd_in.at[which, here, :], wd.at[slot], weight_sem.at[slot, 2]),
        ]

    for copy in tiles(0):
        copy.start()
    plain = [pltpu.make_async_copy(a1_in, a, load_sem.at[0]), pltpu.make_async_copy(dy_in.at[0], dy, load_sem.at[1])]
    turned = [pltpu.make_async_copy(a1t_in, at, load_sem.at[2]), pltpu.make_async_copy(dyt_in, dyt, load_sem.at[3])]
    between = [pltpu.make_async_copy(src, dst, load_sem.at[i]) for i, (src, dst) in enumerate([(h_in, a), (a0t_in, at), (a0_in, a)])]
    for copy in plain + turned:
        copy.start()
    by_gate[...] = jnp.zeros_like(by_gate)
    by_up[...] = jnp.zeros_like(by_up)
    for copy in plain:
        copy.wait()
    pl.semaphore_wait(barrier, 2)

    def serve(turn, odd):
        for age in reversed(range(odd, n)):
            step = 2 * age - odd
            piece = turn - age

            @pl.when(jnp.logical_and(piece >= 0, piece < (pieces if step < n else ringed)))
            def _():
                slot = lax.rem(piece, n)
                copy_of = functools.partial(ring_copy, n, me, slot=slot, own=own, landed=landed, send_sem=send_sem, recv_sem=recv_sem)
                for d in range(2):
                    if step:
                        before = copy_of(d, step - 1, whole=step >= n)
                        before.wait_recv()
                        before.wait_send()
                    mine = ring_rows(n, me, d, step, slot, own)
                    if 0 < step < n:
                        mine[...] = (mine[...].astype(F32) + landed[d, slot, step - 1].astype(F32)).astype(BF16)
                    if step < n - 1:
                        copy_of(d, step, whole=False).start()
                    elif step > n - 1 and step < 2 * n - 2:
                        copy_of(d, step, whole=True).start()
                    elif step == n - 1:

                        @pl.when(piece < ringed)
                        def _():
                            copy_of(d, step, whole=True).start()

                        @pl.when(piece >= ringed)
                        def _():
                            at_out = piece - ringed
                            pltpu.make_async_copy(mine, direct_out.at[at_out, d], direct_sem.at[at_out, d]).start()

                if step == 2 * n - 2:
                    pltpu.make_async_copy(own.at[slot], ring_out.at[piece], out_sem.at[slot]).start()

    @pl.loop(0, max(pieces + n // 2, ringed + n - 1))
    def _(turn):
        busy = turn < pieces
        slot = lax.rem(turn, n)
        now = lax.rem(turn, 2)

        @pl.when(turn == per)
        def _():
            between[0].wait()
            between[1].start()

            @pl.loop(0, tokens // TILE)
            def _(c):
                here = pl.ds(pl.multiple_of(c * TILE, TILE), TILE)
                by_a = (by_gate[here, :].astype(BF16) + by_up[here, :].astype(BF16)).astype(F32)
                wide = a[here, :].astype(F32)
                scale = scale_of(wide)
                along = jnp.mean(by_a * wide, -1, keepdims=True)
                by_h = (by_a * scale - wide * (scale * scale * scale * along)).astype(BF16) + dy[here, :]
                dy[here, :] = by_h
                dyt[:, here] = by_h.T

            between[2].start()
            serve(turn, 1)
            between[1].wait()
            between[2].wait()

        @pl.when(busy)
        def _():
            for copy in tiles(turn):
                copy.wait()

            @pl.when(turn + 1 < pieces)
            def _():
                for copy in tiles(turn + 1):
                    copy.start()

            for at_row in range(0, tokens, ROWS):
                here = pl.ds(at_row, ROWS)
                gate = dot(a[here, :], wg[now])
                up = dot(a[here, :], wu[now])
                by_act = dot_nt(dy[here, :], wd[now]).astype(BF16).astype(F32)
                sig = jax.nn.sigmoid(gate)
                silu = gate * sig
                act[here, :] = (silu * up).astype(BF16)
                dup[here, :] = (by_act * silu).astype(BF16)
                dgate[here, :] = (by_act * up * (sig + silu * (1 - sig))).astype(BF16)

        @pl.when(turn == per - 1)
        def _():
            between[0].start()

        pl.when(turn != per)(functools.partial(serve, turn, 1))

        @pl.when(turn == 0)
        def _():
            for copy in turned:
                copy.wait()

        @pl.when(busy)
        def _():
            @pl.when(turn >= n)
            def _():
                pltpu.make_async_copy(own.at[slot], ring_out.at[0], out_sem.at[slot]).wait()

            own[slot, :d_model, :] = dot(at[...], dgate[...]).astype(BF16)
            own[slot, d_model : 2 * d_model, :] = dot(at[...], dup[...]).astype(BF16)
            down = dot(dyt[...], act[...]).astype(BF16).T
            for i in range(d_model // TILE):
                own[slot, 2 * d_model + i * TILE : 2 * d_model + (i + 1) * TILE, :] = down[:, i * TILE : (i + 1) * TILE]

        def by_input():
            @pl.loop(0, tokens // ROWS)
            def _(c):
                here = pl.ds(pl.multiple_of(c * ROWS, ROWS), ROWS)
                by_gate[here, :] += dot_nt(dgate[here, :], wg[now])
                by_up[here, :] += dot_nt(dup[here, :], wu[now])

        pl.when(jnp.logical_and(turn > 0, turn < per))(by_input)
        serve(turn, 0)
        pl.when(turn == 0)(by_input)

    for piece in range(pieces - n, ringed):
        pltpu.make_async_copy(own.at[piece % n], ring_out.at[piece], out_sem.at[piece % n]).wait()
    for piece in range(ringed, pieces):
        for d in range(2):
            rows = own.at[piece % n, : own.shape[1] // (2 * n), :]
            pltpu.make_async_copy(rows, direct_out.at[piece - ringed, d], direct_sem.at[piece - ringed, d]).wait()


def backward(n, x, dy, h1, a1, a1t, a0, a0t, dyt, wg, wu, wd):
    tokens, d = a1.shape
    ff = wg.shape[2]
    pieces = 2 * ff // TILE
    ringed = pieces - DIRECT
    high = 3 * d // (2 * n)
    anywhere = pl.BlockSpec(memory_space=pl.ANY)
    return pl.pallas_call(
        functools.partial(backward_kernel, n, ringed),
        in_specs=[anywhere] * 10,
        out_specs=[anywhere] * 2,
        out_shape=[jax.ShapeDtypeStruct((ringed, 3 * d, TILE), BF16), jax.ShapeDtypeStruct((DIRECT, 2, high, TILE), BF16)],
        scratch_shapes=[
            pltpu.VMEM((tokens, d), BF16),
            pltpu.VMEM((d, tokens), BF16),
            pltpu.VMEM((tokens, d), BF16),
            pltpu.VMEM((d, tokens), BF16),
            pltpu.VMEM((tokens, d), F32),
            pltpu.VMEM((tokens, d), F32),
            pltpu.VMEM((n, 3 * d, TILE), BF16),
            pltpu.VMEM((2, n, n - 1, high, TILE), BF16),
            pltpu.VMEM((tokens, TILE), BF16),
            pltpu.VMEM((tokens, TILE), BF16),
            pltpu.VMEM((tokens, TILE), BF16),
            pltpu.VMEM((2, d, TILE), BF16),
            pltpu.VMEM((2, d, TILE), BF16),
            pltpu.VMEM((2, TILE, d), BF16),
            pltpu.SemaphoreType.DMA((4,)),
            pltpu.SemaphoreType.DMA((2, 3)),
            pltpu.SemaphoreType.DMA((n,)),
            pltpu.SemaphoreType.DMA((DIRECT, 2)),
            pltpu.SemaphoreType.DMA((2, n)),
            pltpu.SemaphoreType.DMA((2, n, 2 * n - 2)),
        ],
        compiler_params=pltpu.CompilerParams(vmem_limit_bytes=63 * 1024 * 1024, collective_id=0, has_side_effects=True),
        cost_estimate=pl.CostEstimate(flops=28 * tokens * d * ff, bytes_accessed=40 * d * ff, transcendentals=2 * tokens * ff),
        name="backward",
    )(a1, a1t, dy, dyt, h1, a0, a0t, wg, wu, wd)


def adamw_kernel(*refs):
    ins, shards, outs, whole = refs[:9], refs[9], refs[-10:-1], refs[-1]
    d = ins[0].shape[1]
    if len(shards.shape) == 3:
        g_ref = shards.at[0]
    else:
        g_ref, (n, _, _, high, _) = whole, shards.shape
        for q in range(n):
            g_ref[2 * q * high : (2 * q + 1) * high, :] = shards[(q - 1) % n, 0, 0]
            g_ref[(2 * q + 1) * high : (2 * q + 2) * high, :] = shards[(q + 1) % n, 0, 1]
    for i in range(3):
        w, m, v = (ins[3 * k + i] for k in range(3))
        if i < 2:
            g = g_ref[i * d : (i + 1) * d, :].astype(F32)
        else:
            g = jnp.concatenate([g_ref[at : at + TILE, :].astype(F32) for at in range(2 * d, 3 * d, TILE)], axis=1)
        new_m = 0.9 * m[0] + 0.1 * g
        new_v = 0.95 * v[0] + 0.05 * g * g
        step = new_m * lax.rsqrt(new_v + 1e-8) + 0.1 * w[0].astype(F32)
        outs[i][0] = (w[0].astype(F32) - 0.02 * step).astype(BF16)
        outs[3 + i][0] = new_m
        outs[6 + i][0] = new_v


def adamw(weights, ms, vs, g, so_far, first):
    d, ff = weights[0].shape[1:]
    per = ff // TILE
    which = lambda i: 1 - (first + i) // per
    col = pl.BlockSpec((1, d, TILE), lambda i: (which(i), 0, (first + i) % per))
    row = pl.BlockSpec((1, TILE, d), lambda i: (which(i), (first + i) % per, 0))
    three = [col, col, row]
    old = list(so_far or ())
    count = g.size
    if g.ndim == 3:
        number, spec = g.shape[0], pl.BlockSpec((1, 3 * d, TILE), lambda i: (i, 0, 0))
    else:
        number, spec = g.shape[1], pl.BlockSpec((g.shape[0], 1, *g.shape[2:]), lambda i: (0, i, 0, 0, 0))
    return pl.pallas_call(
        adamw_kernel,
        grid=(number,),
        in_specs=three * 3 + [spec] + [pl.BlockSpec(memory_space=pl.ANY)] * len(old),
        out_specs=three * 3,
        out_shape=[jax.ShapeDtypeStruct(v.shape, v.dtype) for v in (*weights, *ms, *vs)],
        input_output_aliases={10 + i: i for i in range(len(old))},
        scratch_shapes=[pltpu.VMEM((3 * d, TILE), BF16)],
        compiler_params=pltpu.CompilerParams(vmem_limit_bytes=LIMIT),
        cost_estimate=pl.CostEstimate(flops=15 * count, bytes_accessed=22 * count, transcendentals=count),
        name=f"adamw_{first}",
    )(*weights, *ms, *vs, g, *old)


def solution(mesh):
    n = mesh.shape["dp"]

    def step(x, dy, *arrays):
        weights, ms, vs = (arrays[i : i + 3] for i in (0, 3, 6))
        wg, wu, wd = weights
        h1, a1, a1t, a0, a0t, dyt = forward(x, dy, wg, wu, wd, 0)
        ring, direct = backward(n, x, dy, h1, a1, a1t, a0, a0t, dyt, wg, wu, wd)
        direct = lax.all_gather(direct, "dp")
        so_far = adamw(weights, ms, vs, ring, None, 0)
        return tuple(adamw(weights, ms, vs, direct, so_far, ring.shape[0]))

    return jax.shard_map(
        step,
        mesh=mesh,
        in_specs=(P(("rep", "dp"), None, None),) * 2 + (P(None, None, None),) * 9,
        out_specs=(P("rep", None, None),) * 9,
        check_vma=False,
    )
```
